32 devices in a mesh: det: 4 (over y, x), tm: 8 (over z, core).
Axes of the slice: x: 2, y: 2, z: 4, core: 2. Of those that a mesh axis runs over, the one named last changes fastest.
Arguments:
- sol_map: float32 [3, 49152], P(None, ('det', 'tm')), may hold values from -6 to 6
- resid_map: float32 [3, 49152], P(None, ('det', 'tm')), may hold values from -6 to 6
- direction: float32 [3, 49152], P(None, ('det', 'tm')), may hold values from -6 to 6
- precond: float32 [3, 49152], P(None, ('det', 'tm')), may hold values from 0.1 to 1
- pixels: int32 [128, 65536], P('det', 'tm'), may hold values from 0 to 49151
- angle_index: int32 [128, 65536], P('det', 'tm'), may hold values from 0 to 127
- angles: float32 [128], replicated, may hold values from -3.140625 to 3.140625
- flag_mask: int32 [128, 65536], P('det', 'tm'), may hold values 0 or 1
- inv_noise: float32 [128, 32769], P(('det', 'tm')), may hold values from 0.05 to 1
Outputs:
- new_sol: float32 [3, 49152], P(None, ('det', 'tm'))
- new_resid: float32 [3, 49152], P(None, ('det', 'tm'))
- new_dir: float32 [3, 49152], P(None, ('det', 'tm'))
- new_norm: float32 [], replicated
The draws below stay inside these ranges and needn't reach their ends.
All inputs are finite; a program needn't handle non-finite values. No bound on the sum of `flag_mask` on one device may be relied on, other than what follows from the above.
Results may differ from the reference program's by a relative error of at most 0.0001.
Values sent between devices are 32-bit elements; how exact they have to be, the bound alone decides.
A program may use at most 320 MiB of HBM per device.

```python
import math
import jax
import jax.numpy as jnp
from jax import lax

NSAMP = 65536
NDET = 128
NPIX = 49152
NANG = 128
NFREQ = 32769


def touch_ends(values, own_key, smallest, largest):
    shape = values.shape
    index_at = [jax.random.randint(jax.random.fold_in(own_key, axis), (), 0, shape[axis]) for axis in range(len(shape))]
    values = values.at[tuple(index_at)].set(smallest)
    longest = shape.index(max(shape))
    index_at[longest] = (index_at[longest] + 1) % shape[longest]
    return values.at[tuple(index_at)].set(largest)


def block_scale(key, dims, cuts, smallest, largest):
    def one(dim, parts):
        heights = jax.random.uniform(jax.random.fold_in(jax.random.fold_in(key, 6), dim), (parts,), jnp.float32, smallest / len(cuts), largest / len(cuts))
        return jnp.repeat(jnp.exp(heights), dims[dim] // parts).reshape((-1,) + (1,) * (len(dims) - dim - 1))

    loudness = one(*cuts[0])
    for cut in cuts[1:]:
        loudness = loudness * one(*cut)
    return loudness


def bell_draw(rng, dims, spread, limit, split=(), kind=jnp.bfloat16):
    values = jax.random.normal(rng, dims, jnp.float32) * spread
    if len(split) > 0:
        values = block_scale(rng, dims, split, -0.22, 0.18) * values
    return jnp.clip(values, min=-limit, max=limit).astype(kind)


def setup_inputs(seed: int = 0) -> dict:
    key_of = jax.random.split(jax.random.key(seed), 10)
    return {
        "sol_map": bell_draw(key_of[0], (3, NPIX), 1.0, 6.0, ((1, 32),), jnp.float32),
        "resid_map": bell_draw(key_of[1], (3, NPIX), 1.0, 6.0, ((1, 32),), jnp.float32),
        "direction": bell_draw(key_of[2], (3, NPIX), 1.0, 6.0, ((1, 32),), jnp.float32),
        "precond": jnp.clip(jnp.exp(math.log(1.0) - 2.3025851 * jax.random.uniform(key_of[3], (3, NPIX), jnp.float32) ** block_scale(key_of[3], (3, NPIX), ((1, 32),), -0.2, 0.2)), 0.1, 1.0),
        "pixels": touch_ends(jax.random.randint(key_of[4], (NDET, NSAMP), 0, NPIX), jax.random.fold_in(key_of[4], 1), 0, NPIX - 1).astype(jnp.int32),
        "angle_index": touch_ends(jax.random.randint(key_of[5], (NDET, NSAMP), 0, NANG), jax.random.fold_in(key_of[5], 1), 0, NANG - 1).astype(jnp.int32),
        "angles": jnp.clip(jax.random.uniform(key_of[6], (NANG,), jnp.float32, -3.140625, 3.140625), -3.140625, 3.140625),
        "flag_mask": touch_ends((jax.random.randint(key_of[7], (NDET, NSAMP), 0, 16) < 15).astype(jnp.int32), jax.random.fold_in(key_of[7], 1), 0, 1),
        "inv_noise": jnp.clip(jnp.exp(math.log(1.0) - 2.9957323 * jax.random.uniform(key_of[8], (NDET, NFREQ), jnp.float32) ** block_scale(key_of[8], (NDET, NFREQ), ((0, 32),), -0.2, 0.2)), 0.05, 1.0),
    }


def reference(sol_map, resid_map, direction, precond, pixels, angle_index, angles, flag_mask, inv_noise):
    cos_table = jnp.cos(2.0 * angles)
    sin_table = jnp.sin(2.0 * angles)
    row_block = 64

    def one_block(image, block_id):
        head_row = block_id * row_block
        pix_rows = lax.dynamic_slice_in_dim(pixels, head_row, row_block, 0)
        ang_rows = lax.dynamic_slice_in_dim(angle_index, head_row, row_block, 0)
        usable = lax.dynamic_slice_in_dim(flag_mask, head_row, row_block, 0).astype(jnp.float32)
        filt_rows = lax.dynamic_slice_in_dim(inv_noise, head_row, row_block, 0)
        cos_two = cos_table[ang_rows]
        sin_two = sin_table[ang_rows]
        signal = usable * (direction[0][pix_rows] + direction[1][pix_rows] * cos_two + direction[2][pix_rows] * sin_two)
        spectrum = jnp.fft.rfft(signal, axis=1)
        filtered = jnp.fft.irfft(spectrum * filt_rows, n=NSAMP, axis=1).astype(jnp.float32)
        weighted = usable * filtered
        contrib = jnp.stack([weighted, weighted * cos_two, weighted * sin_two]).reshape(3, -1)
        image = image.at[:, pix_rows.reshape(-1)].add(contrib)
        return image, None

    image, _ = lax.scan(one_block, jnp.zeros((3, NPIX), jnp.float32), jnp.arange(NDET // row_block, dtype=jnp.int32))
    norm_old = jnp.sum(resid_map * precond * resid_map)
    curvature = jnp.sum(direction * image)
    step_size = norm_old / curvature
    new_sol = sol_map + step_size * direction
    new_resid = resid_map - step_size * image
    new_norm = jnp.sum(new_resid * precond * new_resid)
    new_dir = precond * new_resid + (new_norm / norm_old) * direction
    return new_sol, new_resid, new_dir, new_norm
```

```python
import functools
import math

import jax
import jax.numpy as jnp
from jax import lax
from jax.experimental import pallas as pl
from jax.experimental.pallas import tpu as pltpu
from jax.sharding import PartitionSpec as P

LOW = 256
ROWS = 8
PACK = 16
LANES = 128
WIDTH = 512


def product(form, left, right, precision=lax.Precision.HIGH):
    return jnp.einsum(form, left, right, precision=precision)


def split_two(values):
    upper = values.astype(jnp.bfloat16)
    lower = (values - upper.astype(jnp.float32)).astype(jnp.bfloat16)
    return upper, lower


def lookup(table_row, index):
    rows, width = index.shape
    table = jnp.broadcast_to(table_row, (rows, LANES))
    parts = []
    for start in range(0, width, LANES):
        parts.append(jnp.take_along_axis(table, index[:, start : start + LANES], axis=1, mode="promise_in_bounds"))
    return jnp.concatenate(parts, axis=1)


def one_hot(row, size):
    ids = lax.broadcasted_iota(jnp.int32, (size, row.shape[1]), 0)
    return jnp.where(ids == row, 1.0, 0.0).astype(jnp.bfloat16)


def read_kernel(trig_ref, table_ref, pix_ref, ang_ref, flag_ref, out_ref, split_ref, *, high):
    @pl.when(pl.program_id(0) * pl.num_programs(1) + pl.program_id(1) == 0)
    def _():
        upper, lower = split_two(table_ref[...])
        split_ref[:, :LOW] = upper
        split_ref[:, LOW:] = lower

    cos_two = lookup(trig_ref[0:1, :], ang_ref[...])
    sin_two = lookup(trig_ref[1:2, :], ang_ref[...])
    usable = flag_ref[...].astype(jnp.float32)
    pix = pix_ref[...]
    pix_low = pix & (LOW - 1)
    pix_high = pix // LOW if LOW & (LOW - 1) else pix >> (LOW.bit_length() - 1)
    width = pix.shape[1]
    ids = lax.broadcasted_iota(jnp.int32, (high, width), 0)
    for row in range(ROWS):
        hot = one_hot(pix_low[row : row + 1], LOW)
        got = jnp.dot(split_ref[...], jnp.concatenate([hot, hot], axis=0), preferred_element_type=jnp.float32)
        mixed = got[:high] + got[high : 2 * high] * cos_two[row : row + 1] + got[2 * high :] * sin_two[row : row + 1]
        picked = jnp.sum(jnp.where(ids == pix_high[row : row + 1], mixed, 0.0), axis=0, keepdims=True)
        out_ref[row : row + 1, :] = picked * usable[row : row + 1]


def bin_kernel(trig_ref, pix_ref, ang_ref, flag_ref, val_ref, out_ref, *, high):
    step = pl.program_id(0) * pl.num_programs(1) + pl.program_id(1)

    @pl.when(step == 0)
    def _():
        out_ref[...] = jnp.zeros_like(out_ref)

    cos_two = lookup(trig_ref[0:1, :], ang_ref[...])
    sin_two = lookup(trig_ref[1:2, :], ang_ref[...])
    weighted = flag_ref[...].astype(jnp.float32) * val_ref[...]
    pieces = []
    for stokes in (weighted, weighted * cos_two, weighted * sin_two):
        upper = stokes.astype(jnp.bfloat16).astype(jnp.float32)
        pieces.append((upper, stokes - upper))
    pix = pix_ref[...]
    pix_low = pix & (LOW - 1)
    pix_high = pix >> (LOW.bit_length() - 1)
    total = None
    for row in range(ROWS):
        hot_low = one_hot(pix_low[row : row + 1], LOW)
        hot_high = one_hot(pix_high[row : row + 1], high)
        hot_high = hot_high.reshape(high // PACK, PACK, hot_high.shape[1])
        stack = []
        for part in range(2):
            for stokes in range(3):
                value = pieces[stokes][part][row : row + 1]
                value = jnp.broadcast_to(value, (PACK, value.shape[1])).astype(jnp.bfloat16)
                stack.append((hot_high * value[None]).reshape(high, value.shape[1]))
        left = jnp.concatenate(stack, axis=0)
        got = lax.dot_general(left, hot_low, (((1,), (1,)), ((), ())), preferred_element_type=jnp.float32)
        total = got if total is None else total + got
    out_ref[...] += total


def read_map(trig, table, pixels, angle_index, flag_mask):
    n_det, n_samp = pixels.shape
    high = table.shape[0] // 3
    block = pl.BlockSpec((ROWS, WIDTH), lambda i, j: (i, j))
    fixed = lambda shape: pl.BlockSpec(shape, lambda i, j: (0, 0))
    return pl.pallas_call(
        functools.partial(read_kernel, high=high),
        out_shape=jax.ShapeDtypeStruct((n_det, n_samp), jnp.float32),
        grid=(n_det // ROWS, n_samp // WIDTH),
        in_specs=[fixed(trig.shape), fixed(table.shape), block, block, block],
        out_specs=block,
        scratch_shapes=[pltpu.VMEM((3 * high, 2 * LOW), jnp.bfloat16)],
        compiler_params=pltpu.CompilerParams(dimension_semantics=("arbitrary", "arbitrary")),
        name="read_map",
    )(trig, table, pixels, angle_index, flag_mask)


def bin_map(trig, pixels, angle_index, flag_mask, values, high):
    n_det, n_samp = pixels.shape
    block = pl.BlockSpec((ROWS, WIDTH), lambda i, j: (i, j))
    fixed = lambda shape: pl.BlockSpec(shape, lambda i, j: (0, 0))
    pieces = pl.pallas_call(
        functools.partial(bin_kernel, high=high),
        out_shape=jax.ShapeDtypeStruct((6 * high, LOW), jnp.float32),
        grid=(n_det // ROWS, n_samp // WIDTH),
        in_specs=[fixed(trig.shape), block, block, block, block],
        out_specs=fixed((6 * high, LOW)),
        compiler_params=pltpu.CompilerParams(dimension_semantics=("arbitrary", "arbitrary")),
        name="bin_map",
    )(trig, pixels, angle_index, flag_mask, values)
    return pieces[: 3 * high] + pieces[3 * high :]


def mirrored(filt, side_len):
    n_series, half_len = filt.shape
    rows = (half_len - 1) // side_len
    lower = filt[:, : half_len - 1].reshape(n_series, rows, side_len)
    shifted = filt[:, 1:].reshape(n_series, rows, side_len)
    swap_col = jnp.flip(jnp.eye(side_len, dtype=jnp.float32), 0)
    swap_row = jnp.flip(jnp.eye(rows, dtype=jnp.float32), 0)
    exact = lax.Precision.HIGHEST
    upper = product("wv,dvk->dwk", swap_row, product("dvk,kl->dvl", shifted, swap_col, exact), exact)
    return jnp.concatenate([lower, upper], axis=1)


def noise_weight(series, filt):
    n_series, total_len = series.shape
    side_len = math.isqrt(total_len)
    indices = jnp.arange(side_len, dtype=jnp.int32)
    products = indices[:, None] * indices[None, :]
    angle_tab = 2.0 * math.pi / side_len * (products % side_len).astype(jnp.float32)
    f_real = jnp.cos(angle_tab)
    f_imag = -jnp.sin(angle_tab)
    twist = products.astype(jnp.float32) * (2.0 * math.pi / total_len)
    w_real = jnp.cos(twist)
    w_imag = -jnp.sin(twist)
    matrix_form = series.reshape(n_series, side_len, side_len)
    y_real = product("kt,dtu->dku", f_real, matrix_form)
    y_imag = product("kt,dtu->dku", f_imag, matrix_form)
    y_real, y_imag = (y_real * w_real - y_imag * w_imag, y_real * w_imag + y_imag * w_real)
    z_real = product("dku,uv->dvk", y_real, f_real) - product("dku,uv->dvk", y_imag, f_imag)
    z_imag = product("dku,uv->dvk", y_real, f_imag) + product("dku,uv->dvk", y_imag, f_real)
    weight = mirrored(filt, side_len)
    z_real = z_real * weight
    z_imag = z_imag * weight
    v_real = product("dvk,vu->dku", z_real, f_real) + product("dvk,vu->dku", z_imag, f_imag)
    v_imag = product("dvk,vu->dku", z_imag, f_real) - product("dvk,vu->dku", z_real, f_imag)
    v_real, v_imag = (v_real * w_real + v_imag * w_imag, v_imag * w_real - v_real * w_imag)
    result = product("tk,dku->dtu", f_real, v_real) + product("tk,dku->dtu", f_imag, v_imag)
    return (result / total_len).reshape(n_series, total_len)


def body(sol_map, resid_map, direction, precond, pixels, angle_index, angles, flag_mask, inv_noise):
    everyone = ("det", "tm")
    share_len = direction.shape[1]
    n_dev = lax.axis_size(everyone)
    copies = jnp.broadcast_to(direction.reshape(1, -1, LANES), (n_dev, direction.size // LANES, LANES))
    gathered = lax.all_to_all(copies, everyone, split_axis=0, concat_axis=0, tiled=True)
    high = n_dev * share_len // LOW
    table = jnp.swapaxes(gathered.reshape(n_dev, 3, share_len), 0, 1).reshape(3 * high, LOW)
    trig = jnp.stack([jnp.cos(2.0 * angles), jnp.sin(2.0 * angles)])
    signal = read_map(trig, table, pixels, angle_index, flag_mask)
    by_detector = lax.all_to_all(signal, "tm", split_axis=0, concat_axis=1, tiled=True)
    filtered = noise_weight(by_detector, inv_noise)
    returned = lax.all_to_all(filtered, "tm", split_axis=1, concat_axis=0, tiled=True)
    partial_map = bin_map(trig, pixels, angle_index, flag_mask, returned, high)
    by_owner = jnp.swapaxes(partial_map.reshape(3, n_dev, share_len), 0, 1)
    image = jnp.sum(lax.all_to_all(by_owner, everyone, split_axis=0, concat_axis=0, tiled=True), axis=0)
    scaled_resid = precond * resid_map
    own_sums = jnp.stack(
        [
            jnp.sum(scaled_resid * resid_map),
            jnp.sum(direction * image),
            jnp.sum(image * scaled_resid),
            jnp.sum(image * precond * image),
        ]
    )
    sum_copies = jnp.broadcast_to(own_sums[None], (n_dev, own_sums.shape[0]))
    all_sums = lax.all_to_all(sum_copies, everyone, split_axis=0, concat_axis=0, tiled=True)
    norm_old, curvature, cross_term, image_norm = jnp.sum(all_sums, axis=0)
    step_size = norm_old / curvature
    new_resid = resid_map - step_size * image
    new_norm = norm_old - 2.0 * step_size * cross_term + step_size * step_size * image_norm
    new_sol = sol_map + step_size * direction
    new_dir = precond * new_resid + new_norm / norm_old * direction
    return (new_sol, new_resid, new_dir, new_norm)


def solution(mesh):
    in_specs = (
        P(None, ("det", "tm")),
        P(None, ("det", "tm")),
        P(None, ("det", "tm")),
        P(None, ("det", "tm")),
        P("det", "tm"),
        P("det", "tm"),
        P(),
        P("det", "tm"),
        P(("det", "tm"), None),
    )
    out_specs = (P(None, ("det", "tm")), P(None, ("det", "tm")), P(None, ("det", "tm")), P())
    return jax.shard_map(body, mesh=mesh, in_specs=in_specs, out_specs=out_specs, check_vma=False)
```
